128 devices in a mesh: row: 8 (over z, core), col: 16 (over y, x).
Axes of the slice: x: 4, y: 4, z: 4, core: 2. Of those that a mesh axis runs over, the one named last changes fastest.
Arguments:
- coefs: float32 [2, 1536, 16384], P(None, 'row', 'col'), may hold values from -600 to 600, as said below
- tilts: int32 [1536, 2], replicated, may hold values from 8 to 48
- start_basis: float32 [1536, 32], P('col'), may hold values from -6 to 6
Outputs:
- ccc: float32 [1536, 1536], P('row', 'col')
- basis: float32 [1536, 32], P('col')
The draws below stay inside these ranges and needn't reach their ends.
Inputs may be any that keep to these rules, and one draw needn't show every extreme that they name: `coefs`: real and imaginary parts are products of a particle scale, a coefficient scale and a bounded random value.
All inputs are finite; a program needn't handle non-finite values.
Results may differ from the reference program's by a relative error of at most 0.0003.
Values sent between devices are 32-bit elements; how exact they have to be, the bound alone decides.
No kernel may reach another device: no remote copies, remote signals or barrier semaphores. Data moves between devices by JAX's collectives and lax.ppermute only.
A program may use at most 192 MiB of HBM per device.

```python
import math
import jax
import jax.numpy as jnp
from jax import lax

GRID = 32
K = 16384
P_SIZE = 1536
EIG = 32
ITERS = 4


def draw_coefs(key, part):
    first = jax.random.fold_in(key, 11)
    second = jax.random.fold_in(key, 12)
    third = jax.random.fold_in(key, 13)
    fourth = jax.random.fold_in(key, 14)
    scale_p = jnp.exp(jax.random.uniform(first, (1, P_SIZE, 1), jnp.float32) * math.log(10.0))
    scale_k = jnp.exp(jax.random.uniform(second, (1, 1, K), jnp.float32) * math.log(10.0))
    template = jnp.clip(jax.random.normal(third, (2, 1, K), jnp.float32), -5.0, 5.0)
    noise = jnp.clip(jax.random.normal(fourth, (2, P_SIZE, K), jnp.float32), -5.0, 5.0)
    weight = 0.1
    return (scale_p * scale_k * (noise + weight * template)).astype(jnp.float32)


def plant(result, own_key, smallest, largest):
    shape = result.shape
    spot = [jax.random.randint(jax.random.fold_in(own_key, axis), (), 0, shape[axis]) for axis in range(len(shape))]
    result = result.at[tuple(spot)].set(smallest)
    longest = shape.index(max(shape))
    spot[longest] = (spot[longest] + 1) % shape[longest]
    return result.at[tuple(spot)].set(largest)


def block_scale(key, dims, shards, smallest, largest):
    def one(dim, blocks):
        draws = jax.random.uniform(jax.random.fold_in(jax.random.fold_in(key, 6), dim), (blocks,), jnp.float32, smallest / len(shards), largest / len(shards))
        return jnp.repeat(jnp.exp(draws), dims[dim] // blocks).reshape((-1,) + (1,) * (len(dims) - dim - 1))

    level = one(*shards[0])
    for cut in shards[1:]:
        level = level * one(*cut)
    return level


def gaussian(stream_key, shape, width, most, pieces=(), kind=jnp.bfloat16):
    array = jax.random.normal(stream_key, shape, jnp.float32) * width
    if len(pieces) > 0:
        array = block_scale(stream_key, shape, pieces, -0.22, 0.18) * array
    return jnp.clip(array, min=-most, max=most).astype(kind)


def setup_inputs(seed: int = 0) -> dict:
    arg_keys = jax.random.split(jax.random.key(seed), 4)
    return {
        "coefs": draw_coefs(jax.random.fold_in(arg_keys[3], 71), 0),
        "tilts": plant(jax.random.randint(arg_keys[1], (P_SIZE, 2), 8, 49), jax.random.fold_in(arg_keys[1], 1), 8, 48).astype(jnp.int32),
        "start_basis": gaussian(arg_keys[2], (P_SIZE, EIG), 1.0, 6.0, ((0, 16),), jnp.float32),
    }


EPS = 1e-06
HIGH = lax.Precision.HIGHEST

def wedge(tilt_rows, wave_index):
    wave_x = jnp.abs(wave_index // (GRID * (GRID // 2)) - GRID // 2)[None, :]
    wave_z = (wave_index % GRID - GRID // 2)[None, :]
    upward = wave_z * 16 <= tilt_rows[:, 1:2] * wave_x
    downward = -wave_z * 16 <= tilt_rows[:, 0:1] * wave_x
    return jnp.where(wave_z >= 0, upward, downward).astype(jnp.float32)

def inner(left, right):
    return lax.dot_general(left.astype(jnp.float32), right.astype(jnp.float32), (((1,), (1,)), ((), ())), precision=HIGH, preferred_element_type=jnp.float32)

def reference(coefs, tilts, start_basis):
    masks = wedge(tilts, jnp.arange(K, dtype=jnp.int32))
    paired = jnp.concatenate([coefs[0] * masks, coefs[1] * masks], axis=1)
    energy = masks * (coefs[0] * coefs[0] + coefs[1] * coefs[1])
    numer = inner(paired, paired)
    intersection = inner(energy, masks)
    ccc = numer / jnp.sqrt(intersection * intersection.T + EPS)
    current = start_basis
    for step in range(ITERS):
        wide = jnp.dot(ccc.astype(jnp.float32), current.astype(jnp.float32), precision=HIGH, preferred_element_type=jnp.float32)
        gram = lax.dot_general(wide.astype(jnp.float32), wide.astype(jnp.float32), (((0,), (0,)), ((), ())), precision=HIGH, preferred_element_type=jnp.float32)
        factor = jnp.linalg.cholesky(gram)
        current = lax.linalg.triangular_solve(factor, wide, left_side=False, lower=True, transpose_a=True)
    return (ccc, current * jnp.sqrt(jnp.float32(P_SIZE)))
```

```python
import functools
import math

import jax
import jax.numpy as jnp
from jax import lax
from jax.experimental import pallas as pl
from jax.experimental.pallas import tpu as pltpu
from jax.sharding import PartitionSpec as P

GRID = 32
ITERS = 4
EPS = 1e-06
TILE = 128
SLOTS = 128
VMEM_LIMIT = 24 * 1024 * 1024
HIGH = lax.Precision.HIGHEST


def dot(left, right, contract, precision=None):
    dims = (((contract[0],), (contract[1],)), ((), ()))
    return lax.dot_general(left, right, dims, precision=precision, preferred_element_type=jnp.float32)


def halves(array):
    high = array.astype(jnp.bfloat16)
    return high, (array - high.astype(jnp.float32)).astype(jnp.bfloat16)


def product(left, right, contract):
    total = dot(left[0], right[1], contract) + dot(left[1], right[0], contract)
    return total + dot(left[0], right[0], contract)


def waves(index):
    wave_x = jnp.abs(lax.shift_right_arithmetic(index, 9) - GRID // 2)
    wave_z = jnp.bitwise_and(index, GRID - 1) - GRID // 2
    return wave_x.astype(jnp.float32), wave_z.astype(jnp.float32)


def pairs(blocks):
    return [(a, b) for a in range(blocks) for b in range(a, blocks)]


def sums_kernel(base_ref, mine_ref, theirs_ref, tilts_ref, out_ref, high_ref, low_ref):
    parts, _, rows, depth = mine_ref.shape
    half = parts * rows
    blocks = half // TILE
    tiles = len(pairs(blocks))
    base = base_ref[0]
    wave_x, wave_z = waves(base + lax.broadcasted_iota(jnp.int32, (1, depth), 1))
    upper = wave_z >= 0
    need = 16 * jnp.abs(wave_z)
    row_x, row_z = waves(base + lax.broadcasted_iota(jnp.int32, (depth, SLOTS), 0))
    slot = lax.broadcasted_iota(jnp.int32, (depth, SLOTS), 1)
    reach = jnp.where(slot < 64, slot, slot - 64).astype(jnp.float32) * row_x
    table = (16 * jnp.abs(row_z) <= reach) & ((row_z >= 0) == (slot < 64))
    table = jnp.where(table, 1.0, 0.0).astype(jnp.bfloat16)

    for side, ref in enumerate((mine_ref, theirs_ref)):

        def fill(part, _, side=side, ref=ref):
            start = pl.multiple_of(side * half + part * rows, 64)
            tilt = tilts_ref[pl.ds(start, rows), :]
            limit = jnp.where(upper, tilt[:, 1:2], tilt[:, 0:1]) * wave_x
            keep = need <= limit
            energy = None
            for comp in range(2):
                value = jnp.where(keep, ref[part, comp], 0.0)
                high, low = halves(value)
                high_ref[pl.ds(start, rows), comp * depth : (comp + 1) * depth] = high
                low_ref[pl.ds(start, rows), comp * depth : (comp + 1) * depth] = low
                square = value * value
                energy = square if energy is None else energy + square
            if side == 0:
                high, low = halves(energy)
                spread = dot(high, table, (1, 0)) + dot(low, table, (1, 0))
                out_ref[pl.ds(pl.multiple_of(2 * tiles * TILE + start, 64), rows), :] = spread
            return 0

        lax.fori_loop(0, parts, fill, 0)

    where = {pair: k for k, pair in enumerate(pairs(blocks))}
    wide = 2 * TILE
    for side in range(2):
        for a, b in pairs(half // wide):
            left = slice(a * wide, (a + 1) * wide)
            right = slice(side * half + b * wide, side * half + (b + 1) * wide)
            numer = product(
                (high_ref[left, :], low_ref[left, :]), (high_ref[right, :], low_ref[right, :]), (1, 1)
            )
            for i in range(2):
                for j in range(2):
                    if (2 * a + i, 2 * b + j) in where:
                        k = side * tiles + where[2 * a + i, 2 * b + j]
                        out_ref[k * TILE : (k + 1) * TILE, :] = numer[
                            i * TILE : (i + 1) * TILE, j * TILE : (j + 1) * TILE
                        ]


def matrix_kernel(where_ref, all_ref, partner_ref, tilts_ref, start_ref, high_ref, low_ref, block_ref, wide_ref, spread_ref, hot_ref):
    half, total = high_ref.shape
    blocks = half // TILE
    tri = pairs(blocks)
    tiles = len(tri)
    index = {pair: k for k, pair in enumerate(tri)}
    slot = lax.broadcasted_iota(jnp.int32, (total, SLOTS), 1).astype(jnp.float32)
    hot = (slot == tilts_ref[:, 1:2]) | (slot == tilts_ref[:, 0:1] + 64)
    hot = jnp.where(hot, 1.0, 0.0).astype(jnp.bfloat16)
    hot_ref[:, :SLOTS] = hot
    hot_ref[:, SLOTS:] = hot

    def mine(k):
        per = (all_ref.shape[2] - start_rows) // TILE
        piece, rest = divmod(k, per)
        return all_ref[piece // all_ref.shape[1], piece % all_ref.shape[1], rest * TILE : (rest + 1) * TILE, :]

    start_rows = all_ref.shape[2] % TILE
    for b in range(2 * blocks):
        value = mine(2 * tiles + b) if b < blocks else partner_ref[(tiles + b - blocks) * TILE : (tiles + b - blocks + 1) * TILE, :]
        high, low = halves(value)
        spread_ref[b * TILE : (b + 1) * TILE, :SLOTS] = high
        spread_ref[b * TILE : (b + 1) * TILE, SLOTS:] = low
    for a in range(blocks):
        rows = slice(a * TILE, (a + 1) * TILE)
        scale = dot(spread_ref[rows, :], hot_ref[...], (1, 1)) * dot(hot_ref[rows, :], spread_ref[...], (1, 1)) + EPS
        guess = lax.rsqrt(scale)
        guess = guess * (1.5 - 0.5 * (scale * guess) * guess)
        for b in range(2 * blocks):
            if b < blocks:
                numer = mine(index[a, b]) if a <= b else mine(index[b, a]).T
            elif a <= b - blocks:
                numer = mine(tiles + index[a, b - blocks])
            else:
                k = index[b - blocks, a]
                numer = partner_ref[k * TILE : (k + 1) * TILE, :].T
            cols = slice(b * TILE, (b + 1) * TILE)
            high, low = halves(numer * guess[:, cols])
            high_ref[rows, cols] = high
            low_ref[rows, cols] = low
    n_rows, n_cols = block_ref.shape
    first = pl.multiple_of(where_ref[0], 64)
    pick = lax.broadcasted_iota(jnp.int32, (total, TILE), 0) == (
        lax.broadcasted_iota(jnp.int32, (total, TILE), 1) + where_ref[1]
    )
    pick = jnp.where(pick, 1.0, 0.0).astype(jnp.bfloat16)
    picked = dot(high_ref[pl.ds(first, n_rows), :], pick, (1, 0)) + dot(low_ref[pl.ds(first, n_rows), :], pick, (1, 0))
    block_ref[...] = picked[:, :n_cols]
    wide_ref[...] = product((high_ref[...], low_ref[...]), halves(start_ref[...]), (1, 0))


def inverse_factor(gram):
    size = gram.shape[0]
    columns = [jnp.broadcast_to(gram[j // 8 * 8 :, j : j + 1], (size - j // 8 * 8, TILE)) for j in range(size)]
    inverse = jnp.where(
        lax.broadcasted_iota(jnp.int32, (size, TILE), 0) == lax.broadcasted_iota(jnp.int32, (size, TILE), 1), 1.0, 0.0
    )
    rows = lax.broadcasted_iota(jnp.int32, (size, TILE), 0)
    for k in range(size):
        base = k // 8 * 8
        pivot = jnp.broadcast_to(columns[k][k - base : k - base + 1, :], (8, TILE))
        root = lax.rsqrt(pivot)
        root = root * (1.5 - 0.5 * (pivot * root) * root)
        scaled = columns[k] * jnp.broadcast_to(root[:1], columns[k].shape)
        line = inverse[k : k + 1, :] * root[:1]
        below = jnp.where(rows[base:] > k, scaled, 0.0)
        tail = inverse[base:] - below * line
        tail = jnp.where(rows[base:] == k, line, tail)
        inverse = jnp.concatenate([inverse[:base], tail], axis=0) if base else tail
        for j in range(k + 1, size):
            shift = j // 8 * 8 - base
            columns[j] = columns[j] - scaled[shift:] * scaled[j - base : j - base + 1, :]
    return inverse[:, :size]


def normalized(own_ref, other_ref):
    own, other = own_ref[...], other_ref[...]
    gram = dot(own, own, (0, 0), HIGH) + dot(other, other, (0, 0), HIGH)
    inverse = inverse_factor(gram)
    return dot(own, inverse, (1, 1), HIGH), dot(other, inverse, (1, 1), HIGH)


def step_kernel(high_ref, low_ref, own_ref, other_ref, wide_ref):
    half = own_ref.shape[0]
    own, other = normalized(own_ref, other_ref)
    total = 0.0
    for part, cols in ((own, slice(0, half)), (other, slice(half, 2 * half))):
        total = total + product((high_ref[:, cols], low_ref[:, cols]), halves(part), (1, 0))
    wide_ref[...] = total


def last_kernel(own_ref, other_ref, out_ref):
    half = own_ref.shape[0]
    own, other = normalized(own_ref, other_ref)
    scale = math.sqrt(2 * half)
    out_ref[:half, :] = own * scale
    out_ref[half:, :] = other * scale


def call(body, name, out, inputs, scratch=(), flops=10**9, smem=0):
    vmem = pl.BlockSpec(memory_space=pltpu.VMEM)
    specs = [pl.BlockSpec(memory_space=pltpu.SMEM)] * smem + [vmem] * (len(inputs) - smem)
    return pl.pallas_call(
        body,
        name=name,
        out_shape=out,
        in_specs=specs,
        out_specs=jax.tree.map(lambda _: vmem, out),
        scratch_shapes=list(scratch),
        compiler_params=pltpu.CompilerParams(vmem_limit_bytes=VMEM_LIMIT),
        cost_estimate=pl.CostEstimate(flops=flops, bytes_accessed=10**7, transcendentals=0),
    )(*inputs)


def local(coefs, tilts, start_basis, n_z, n_y, n_x):
    _, rows, width = coefs.shape
    cols, eig = start_basis.shape
    n_row, n_col = 2 * n_z, n_y * n_x
    total = rows * n_row
    half = total // 2
    depth = width // n_z
    blocks = half // TILE
    tiles = len(pairs(blocks))
    f32 = functools.partial(jax.ShapeDtypeStruct, dtype=jnp.float32)
    bf16 = functools.partial(jax.ShapeDtypeStruct, dtype=jnp.bfloat16)
    row = lax.axis_index("row")
    col = lax.axis_index("col")
    z = row // 2
    core = row % 2

    def device(a, c, y, x):
        return (2 * a + c) * n_col + y * n_x + x

    along_x = [[[device(a, c, y, x) for x in range(n_x)] for a in range(n_z) for y in range(n_y)] for c in range(2)]
    along_y = [[[device(a, c, y, x) for y in range(n_y)] for a in range(n_z) for x in range(n_x)] for c in range(2)]
    first_groups = along_x[0] + along_y[1]
    second_groups = along_y[0] + along_x[1]
    z_groups = [[2 * a + c for a in range(n_z)] for c in range(2)]
    swap = [(a, a ^ 1) for a in range(n_row)]

    def over_z(array):
        return lax.all_to_all(array, "row", split_axis=0, concat_axis=0, tiled=True, axis_index_groups=z_groups)

    def over(array, groups):
        return lax.all_to_all(
            array, ("row", "col"), split_axis=0, concat_axis=0, tiled=True, axis_index_groups=groups
        )

    def other_core(array):
        return lax.ppermute(array, "row", swap)

    def to_local(array):
        cut = array.reshape(n_z, 2, rows, -1)
        own = lax.dynamic_index_in_dim(cut, core, 1, keepdims=False).reshape(half, -1)
        other = lax.dynamic_index_in_dim(cut, 1 - core, 1, keepdims=False).reshape(half, -1)
        return jnp.concatenate([own, other], axis=0)

    cut = coefs.reshape(2, rows, n_z, depth).transpose(2, 0, 1, 3)
    mine = over_z(cut)
    theirs = other_core(mine)
    tilts_here = to_local(tilts).astype(jnp.float32)
    base = (col * width + z * depth)[None]
    count = 2 * tiles + blocks
    sums = call(
        sums_kernel,
        "sums",
        f32((count * TILE, TILE)),
        (base, mine, theirs, tilts_here),
        (pltpu.VMEM((total, 2 * depth), jnp.bfloat16), pltpu.VMEM((total, 2 * depth), jnp.bfloat16)),
        smem=1,
    )
    sums = over(sums.reshape(n_x, -1, TILE), first_groups).sum(axis=0)
    sums = over(sums.reshape(n_y, -1, TILE), second_groups).sum(axis=0)
    sums = over_z(jnp.broadcast_to(sums, (n_z, *sums.shape))).sum(axis=0)
    packed = jnp.concatenate([sums, start_basis.reshape(-1, TILE)], axis=0)
    line = over(jnp.broadcast_to(packed, (n_y, *packed.shape)), second_groups)
    everyone = over(jnp.broadcast_to(line, (n_x, *line.shape)), first_groups)
    per = sums.shape[0]
    starts = everyone[:, :, per:]
    starts = jnp.where(core == 0, starts.swapaxes(0, 1), starts)
    start = to_local(starts.reshape(total, eig))
    shared = everyone[:, :, :per].reshape(-1, TILE)[tiles * TILE :]
    partner = other_core(shared)
    owner = (col * cols) // rows
    place = jnp.where(owner % 2 == core, 0, half) + (owner // 2) * rows + (col * cols) % rows
    where = jnp.stack([z * rows, place])
    high, low, block, own = call(
        matrix_kernel,
        "matrix",
        (bf16((half, total)), bf16((half, total)), f32((rows, cols)), f32((half, eig))),
        (where, everyone, partner, tilts_here, start),
        (pltpu.VMEM((total, 2 * SLOTS), jnp.bfloat16), pltpu.VMEM((total, 2 * SLOTS), jnp.bfloat16)),
        smem=1,
    )
    other = other_core(own)
    for _ in range(ITERS - 1):
        own = call(step_kernel, "step", f32((half, eig)), (high, low, own, other))
        other = other_core(own)
    basis = call(last_kernel, "last", f32((total, eig)), (own, other))
    basis = lax.dynamic_slice_in_dim(basis, place, cols, 0)
    return (block, basis)


def solution(mesh):
    n_z = mesh.shape["row"] // 2
    side = math.isqrt(mesh.shape["col"])
    in_specs = (P(None, "row", "col"), P(), P("col", None))
    out_specs = (P("row", "col"), P("col", None))
    body = functools.partial(local, n_z=n_z, n_y=side, n_x=side)
    return jax.shard_map(body, mesh=mesh, in_specs=in_specs, out_specs=out_specs, check_vma=False)
```

```python
import functools
import math

import jax
import jax.numpy as jnp
from jax import lax
from jax.experimental import pallas as pl
from jax.experimental.pallas import tpu as pltpu
from jax.sharding import PartitionSpec as P

GRID = 32
ITERS = 4
EPS = 1e-06
TILE = 128
SLOTS = 128
VMEM_LIMIT = 32 * 1024 * 1024
CHUNKS = (3,)
SHARED = 1
ORDER = (2, 1, 3)
HIGH = lax.Precision.HIGHEST


def dot(left, right, contract, precision=None):
    dims = (((contract[0],), (contract[1],)), ((), ()))
    return lax.dot_general(left, right, dims, precision=precision, preferred_element_type=jnp.float32)


def halves(array):
    high = array.astype(jnp.bfloat16)
    return high, (array - high.astype(jnp.float32)).astype(jnp.bfloat16)


def product(left, right, contract):
    total = dot(left[0], right[1], contract) + dot(left[1], right[0], contract)
    return total + dot(left[0], right[0], contract)


def waves(index):
    wave_x = jnp.abs(lax.shift_right_arithmetic(index, 9) - GRID // 2)
    wave_z = jnp.bitwise_and(index, GRID - 1) - GRID // 2
    return wave_x.astype(jnp.float32), wave_z.astype(jnp.float32)


def pairs(blocks):
    return [(a, b) for a in range(blocks) for b in range(a, blocks)]


def tile_order(blocks):
    tri = pairs(blocks)
    order = [("cross", *pair) for pair in tri] + [("spread", a, 0) for a in range(blocks)]
    return order + [("own", *pair) for pair in tri]


def places(blocks, chunks, n_a, n_b):
    found, start = {}, 0
    order = tile_order(blocks)
    for chunk, per in enumerate(chunks):
        for k in range(n_a * n_b * per):
            found[order[start + k]] = (chunk, k // (n_b * per), k // per % n_b, k % per)
        start += n_a * n_b * per
    return found


def split_kernel(where_ref, coefs_ref, *out_refs):
    depth = out_refs[0].shape[2]
    for k, out_ref in enumerate(out_refs):
        first = pl.multiple_of(jnp.bitwise_and(where_ref[0] + k, len(out_refs) - 1) * depth, depth)
        out_ref[...] = coefs_ref[:, :, pl.ds(first, depth)]


def sums_kernel(chunks, n_a, n_b, where_ref, tilts_ref, starts_ref, *refs):
    n = len(chunks)
    value_refs = refs[: -4 - n]
    start_ref, *out_refs = refs[-4 - n : -3]
    high_ref, low_ref, spread_ref = refs[-3:]
    n_z = len(value_refs) // 2
    _, rows, depth = value_refs[0].shape
    cols = starts_ref.shape[1]
    half = n_z * rows
    blocks = half // TILE
    base, z, at_a, at_b, core = (where_ref[k] for k in range(5))
    for col in range(n_a * n_b):
        owner = col * cols // rows
        place = jnp.where(core == owner % 2, 0, half) + (owner // 2 * rows + col * cols % rows)
        start_ref[pl.ds(pl.multiple_of(place, 32), cols), :] = starts_ref[col]
    wave_x, wave_z = waves(base + lax.broadcasted_iota(jnp.int32, (1, depth), 1))
    upper = wave_z >= 0
    need = 16 * jnp.abs(wave_z)
    row_x, row_z = waves(base + lax.broadcasted_iota(jnp.int32, (depth, SLOTS), 0))
    slot = lax.broadcasted_iota(jnp.int32, (depth, SLOTS), 1)
    reach = jnp.where(slot < 64, slot, slot - 64).astype(jnp.float32) * row_x
    table = (16 * jnp.abs(row_z) <= reach) & ((row_z >= 0) == (slot < 64))
    table = jnp.where(table, 1.0, 0.0).astype(jnp.bfloat16)

    for k, ref in enumerate(value_refs):
        side, back = divmod(k, n_z)
        part = jnp.bitwise_and(z - back, n_z - 1) * rows
        start = pl.multiple_of(side * half + part, 64)
        tilt = tilts_ref[pl.ds(pl.multiple_of(2 * part + jnp.bitwise_xor(core, side) * rows, 64), rows), :]
        tilt = tilt.astype(jnp.float32)
        limit = jnp.where(upper, tilt[:, 1:2], tilt[:, 0:1]) * wave_x
        keep = need <= limit
        energy = None
        for comp in range(2):
            value = jnp.where(keep, ref[comp], 0.0)
            high, low = halves(value)
            high_ref[pl.ds(start, rows), comp * depth : (comp + 1) * depth] = high
            low_ref[pl.ds(start, rows), comp * depth : (comp + 1) * depth] = low
            square = value * value
            energy = square if energy is None else energy + square
        if side == 0:
            high, low = halves(energy)
            spread = dot(high, table, (1, 0)) + dot(low, table, (1, 0))
            spread_ref[pl.ds(pl.multiple_of(part, 64), rows), :] = spread

    place = places(blocks, chunks, n_a, n_b)

    def store(name, value):
        if name in place:
            chunk, q_a, q_b, k = place[name]
            a = jnp.bitwise_and(q_a - at_a, n_a - 1)
            b = jnp.bitwise_and(q_b - at_b, n_b - 1)
            out_refs[chunk][a, b, k * TILE : (k + 1) * TILE, :] = value

    for a in range(blocks):
        store(("spread", a, 0), spread_ref[a * TILE : (a + 1) * TILE, :])
    wide = 2 * TILE
    for side, name in ((1, "cross"), (0, "own")):
        for a, b in pairs(half // wide):
            left = slice(a * wide, (a + 1) * wide)
            right = slice(side * half + b * wide, side * half + (b + 1) * wide)
            numer = product(
                (high_ref[left, :], low_ref[left, :]), (high_ref[right, :], low_ref[right, :]), (1, 1)
            )
            for i in range(2):
                for j in range(2):
                    cut = numer[i * TILE : (i + 1) * TILE, j * TILE : (j + 1) * TILE]
                    store((name, 2 * a + i, 2 * b + j), cut)


def matrix_kernel(chunks, shared, n_a, n_b, where_ref, tilts_ref, *refs):
    n = len(chunks)
    own_refs = [refs[c * n_a : (c + 1) * n_a] for c in range(n)]
    partner_refs = [refs[(n + c) * n_a : (n + c + 1) * n_a] for c in range(shared)]
    start_ref, high_ref, low_ref, block_ref, wide_ref = refs[(n + shared) * n_a : (n + shared) * n_a + 5]
    spread_ref, hot_ref, *whole_refs = refs[(n + shared) * n_a + 5 :]
    half, total = high_ref.shape
    blocks = half // TILE
    rows, cols = block_ref.shape
    first, pick_at, at_a, at_b, core = (where_ref[k] for k in range(5))
    for side, sources in enumerate((own_refs, partner_refs)):
        here_a, here_b = (at_a, at_b) if side == 0 else (at_b, at_a)
        for chunk, arrays in enumerate(sources):
            whole_ref = whole_refs[side * n + chunk]
            for a, array in enumerate(arrays):
                for b in range(n_b):
                    slot = jnp.bitwise_and(here_a - a, n_a - 1) * n_b + jnp.bitwise_and(here_b - b, n_b - 1)
                    whole_ref[slot] = array[b]
    place = places(blocks, chunks, n_a, n_b)

    def tile(side, *name):
        chunk, q_a, q_b, k = place[name]
        return whole_refs[side * n + chunk][q_a * n_b + q_b, k * TILE : (k + 1) * TILE, :]

    slot = lax.broadcasted_iota(jnp.int32, (rows, SLOTS), 1)
    for side in range(2):
        for part in range(half // rows):
            tilt = tilts_ref[pl.ds(pl.multiple_of((2 * part + jnp.bitwise_xor(core, side)) * rows, 64), rows), :]
            hot = (slot == tilt[:, 1:2]) | (slot == tilt[:, 0:1] + 64)
            hot = jnp.where(hot, 1.0, 0.0).astype(jnp.bfloat16)
            lines = slice(side * half + part * rows, side * half + (part + 1) * rows)
            hot_ref[lines, :SLOTS] = hot
            hot_ref[lines, SLOTS:] = hot
    for b in range(2 * blocks):
        high, low = halves(tile(b // blocks, "spread", b % blocks, 0))
        spread_ref[b * TILE : (b + 1) * TILE, :SLOTS] = high
        spread_ref[b * TILE : (b + 1) * TILE, SLOTS:] = low
    for a in range(blocks):
        lines = slice(a * TILE, (a + 1) * TILE)
        scale = dot(spread_ref[lines, :], hot_ref[...], (1, 1)) * dot(hot_ref[lines, :], spread_ref[...], (1, 1)) + EPS
        guess = lax.rsqrt(scale)
        guess = guess * (1.5 - 0.5 * (scale * guess) * guess)
        for b in range(2 * blocks):
            if b < blocks:
                numer = tile(0, "own", a, b) if a <= b else tile(0, "own", b, a).T
            else:
                numer = tile(0, "cross", a, b - blocks) if a <= b - blocks else tile(1, "cross", b - blocks, a).T
            across = slice(b * TILE, (b + 1) * TILE)
            high, low = halves(numer * guess[:, across])
            high_ref[lines, across] = high
            low_ref[lines, across] = low
    first = pl.multiple_of(first, 64)
    pick = lax.broadcasted_iota(jnp.int32, (total, TILE), 0) == (
        lax.broadcasted_iota(jnp.int32, (total, TILE), 1) + pick_at
    )
    pick = jnp.where(pick, 1.0, 0.0).astype(jnp.bfloat16)
    picked = dot(high_ref[pl.ds(first, rows), :], pick, (1, 0)) + dot(low_ref[pl.ds(first, rows), :], pick, (1, 0))
    block_ref[...] = picked[:, :cols]
    wide_ref[...] = product((high_ref[...], low_ref[...]), halves(start_ref[...]), (1, 0))


def inverse_factor(gram):
    size = gram.shape[0]
    columns = [jnp.broadcast_to(gram[j // 8 * 8 :, j : j + 1], (size - j // 8 * 8, TILE)) for j in range(size)]
    inverse = jnp.where(
        lax.broadcasted_iota(jnp.int32, (size, TILE), 0) == lax.broadcasted_iota(jnp.int32, (size, TILE), 1), 1.0, 0.0
    )
    rows = lax.broadcasted_iota(jnp.int32, (size, TILE), 0)
    for k in range(size):
        base = k // 8 * 8
        pivot = jnp.broadcast_to(columns[k][k - base : k - base + 1, :], (8, TILE))
        root = lax.rsqrt(pivot)
        root = root * (1.5 - 0.5 * (pivot * root) * root)
        scaled = columns[k] * jnp.broadcast_to(root[:1], columns[k].shape)
        line = inverse[k : k + 1, :] * root[:1]
        below = jnp.where(rows[base:] > k, scaled, 0.0)
        tail = inverse[base:] - below * line
        tail = jnp.where(rows[base:] == k, line, tail)
        inverse = jnp.concatenate([inverse[:base], tail], axis=0) if base else tail
        for j in range(k + 1, size):
            shift = j // 8 * 8 - base
            columns[j] = columns[j] - scaled[shift:] * scaled[j - base : j - base + 1, :]
    return inverse[:, :size]


def normalized(own_ref, other_ref):
    own, other = own_ref[...], other_ref[...]
    gram = dot(own, own, (0, 0), HIGH) + dot(other, other, (0, 0), HIGH)
    inverse = inverse_factor(gram)
    return dot(own, inverse, (1, 1), HIGH), dot(other, inverse, (1, 1), HIGH)


def step_kernel(high_ref, low_ref, own_ref, other_ref, wide_ref):
    half = own_ref.shape[0]
    own, other = normalized(own_ref, other_ref)
    total = 0.0
    for part, cols in ((own, slice(0, half)), (other, slice(half, 2 * half))):
        total = total + product((high_ref[:, cols], low_ref[:, cols]), halves(part), (1, 0))
    wide_ref[...] = total


def last_kernel(own_ref, other_ref, out_ref):
    half = own_ref.shape[0]
    own, other = normalized(own_ref, other_ref)
    scale = math.sqrt(2 * half)
    out_ref[:half, :] = own * scale
    out_ref[half:, :] = other * scale


def call(body, name, out, inputs, scratch=(), flops=10**9, smem=0):
    vmem = pl.BlockSpec(memory_space=pltpu.VMEM)
    specs = [pl.BlockSpec(memory_space=pltpu.SMEM)] * smem + [vmem] * (len(inputs) - smem)
    return pl.pallas_call(
        body,
        name=name,
        out_shape=out,
        in_specs=specs,
        out_specs=jax.tree.map(lambda _: vmem, out),
        scratch_shapes=list(scratch),
        compiler_params=pltpu.CompilerParams(vmem_limit_bytes=VMEM_LIMIT),
        cost_estimate=pl.CostEstimate(flops=flops, bytes_accessed=10**7, transcendentals=0),
    )(*inputs)


def local(coefs, tilts, start_basis, n_z, n_a):
    _, rows, width = coefs.shape
    cols, eig = start_basis.shape
    n_b = n_a
    n_row, n_col = 2 * n_z, n_a * n_b
    total = rows * n_row
    half = total // 2
    depth = width // n_z
    blocks = half // TILE
    f32 = functools.partial(jax.ShapeDtypeStruct, dtype=jnp.float32)
    bf16 = functools.partial(jax.ShapeDtypeStruct, dtype=jnp.bfloat16)
    row = lax.axis_index("row")
    col = lax.axis_index("col")
    z, core = row // 2, row % 2
    y, x = col // n_a, col % n_a
    at_a = jnp.where(core == 0, x, y)
    at_b = jnp.where(core == 0, y, x)

    def device(d, c, q_a, q_b):
        q_a, q_b = q_a % n_a, q_b % n_b
        return (2 * (d % n_z) + c) * n_col + (q_b * n_a + q_a if c == 0 else q_a * n_b + q_b)

    everywhere = [(d, c, a, b) for d in range(n_z) for c in range(2) for a in range(n_a) for b in range(n_b)]

    def send(array, step_a=0, step_b=0, step_z=0):
        perm = [(device(d, c, a, b), device(d + step_z, c, a + step_a, b + step_b)) for d, c, a, b in everywhere]
        return lax.ppermute(array, ("row", "col"), sorted(perm))

    def other_core(array):
        return lax.ppermute(array, "row", [(a, a ^ 1) for a in range(n_row)])

    steps = ORDER
    cut = call(split_kernel, "split", [f32((2, rows, depth))] * n_z, (z[None], coefs), smem=1)
    mine = [cut[0]] + [None] * (n_z - 1)
    for k in steps:
        mine[k] = send(cut[k], step_z=k)
    starts = jnp.broadcast_to(start_basis, (n_col, cols, eig))
    starts = lax.all_to_all(starts, "col", split_axis=0, concat_axis=0, tiled=True)
    mine[0], tilts = lax.optimization_barrier((mine[0], tilts))
    theirs = [other_core(mine[0])]
    *mine[1:], starts = lax.optimization_barrier((*mine[1:], starts))
    theirs += [other_core(array) for array in mine[1:]]
    where = jnp.stack([col * width + z * depth, z, at_a, at_b, core])
    outs = [f32((total, eig))] + [f32((n_a, n_b, per * TILE, TILE)) for per in CHUNKS]
    start, *sums = call(
        functools.partial(sums_kernel, CHUNKS, n_a, n_b),
        "sums",
        outs,
        (where, tilts, starts, *mine, *theirs),
        (
            pltpu.VMEM((total, 2 * depth), jnp.bfloat16),
            pltpu.VMEM((total, 2 * depth), jnp.bfloat16),
            pltpu.VMEM((half, SLOTS), jnp.float32),
        ),
        smem=1,
    )
    gathered, partner = [], []
    arrived = [[send(part[k], step_a=k) for k in steps] for part in sums]
    for chunk, part in enumerate(sums):
        summed = part[0] + sum(arrived[chunk])
        summed = summed[0] + sum(send(summed[k], step_b=k) for k in steps)
        summed = summed + sum(send(summed, step_z=k) for k in steps)
        near = [summed] + [None] * (n_b - 1)
        for k in steps:
            near[k] = send(summed, step_b=k)
        near = jnp.stack(near)
        far = [near] + [None] * (n_a - 1)
        for k in steps:
            far[k] = send(near, step_a=k)
        gathered += far
        if chunk < SHARED:
            partner += [other_core(array) for array in far]
    owner = (col * cols) // rows
    place = jnp.where(owner % 2 == core, 0, half) + (owner // 2) * rows + (col * cols) % rows
    where = jnp.stack([z * rows, place, at_a, at_b, core])
    whole = [pltpu.VMEM((n_col, per * TILE, TILE), jnp.float32) for per in CHUNKS]
    high, low, block, own = call(
        functools.partial(matrix_kernel, CHUNKS, SHARED, n_a, n_b),
        "matrix",
        (bf16((half, total)), bf16((half, total)), f32((rows, cols)), f32((half, eig))),
        (where, tilts, *gathered, *partner, start),
        (
            pltpu.VMEM((total, 2 * SLOTS), jnp.bfloat16),
            pltpu.VMEM((total, 2 * SLOTS), jnp.bfloat16),
            *whole,
            *whole[:SHARED],
        ),
        smem=1,
    )
    other = other_core(own)
    for _ in range(ITERS - 1):
        own = call(step_kernel, "step", f32((half, eig)), (high, low, own, other))
        other = other_core(own)
    basis = call(last_kernel, "last", f32((total, eig)), (own, other))
    basis = lax.dynamic_slice_in_dim(basis, place, cols, 0)
    return (block, basis)


def solution(mesh):
    n_z = mesh.shape["row"] // 2
    side = math.isqrt(mesh.shape["col"])
    in_specs = (P(None, "row", "col"), P(), P("col", None))
    out_specs = (P("row", "col"), P("col", None))
    body = functools.partial(local, n_z=n_z, n_a=side)
    return jax.shard_map(body, mesh=mesh, in_specs=in_specs, out_specs=out_specs, check_vma=False)
```

```python
import functools
import math

import jax
import jax.numpy as jnp
from jax import lax
from jax.experimental import pallas as pl
from jax.experimental.pallas import tpu as pltpu
from jax.sharding import PartitionSpec as P

GRID = 32
ITERS = 4
EPS = 1e-06
TILE = 128
SLOTS = 128
CHUNKS = (3,)
SHARED = 1
ORDER = (2, 1, 3)
HIGH = lax.Precision.HIGHEST


def dot(left, right, contract, precision=None):
    dims = (((contract[0],), (contract[1],)), ((), ()))
    return lax.dot_general(left, right, dims, precision=precision, preferred_element_type=jnp.float32)


def halves(array):
    high = array.astype(jnp.bfloat16)
    return high, (array - high.astype(jnp.float32)).astype(jnp.bfloat16)


def product(left, right, contract):
    total = dot(left[0], right[1], contract) + dot(left[1], right[0], contract)
    return total + dot(left[0], right[0], contract)


def turned(ref):
    rows = ref[...].astype(jnp.float32)
    return jnp.concatenate([rows] * 4, axis=0).T


def waves(index):
    wave_x = jnp.abs(lax.shift_right_arithmetic(index, 9) - GRID // 2)
    wave_z = jnp.bitwise_and(index, GRID - 1) - GRID // 2
    return wave_x.astype(jnp.float32), wave_z.astype(jnp.float32)


def pairs(blocks):
    return [(a, b) for a in range(blocks) for b in range(a, blocks)]


def tile_order(blocks):
    tri = pairs(blocks)
    order = [("cross", *pair) for pair in tri] + [("spread", a, 0) for a in range(blocks)]
    return order + [("own", *pair) for pair in tri]


def places(blocks, chunks, n_a, n_b):
    found, start = {}, 0
    order = tile_order(blocks)
    for chunk, per in enumerate(chunks):
        for k in range(n_a * n_b * per):
            found[order[start + k]] = (chunk, k // (n_b * per), k // per % n_b, k % per)
        start += n_a * n_b * per
    return found


def split_kernel(where_ref, coefs_ref, *out_refs):
    depth = out_refs[0].shape[2]
    for k, out_ref in enumerate(out_refs):
        first = pl.multiple_of(jnp.bitwise_and(where_ref[1] + k, len(out_refs) - 1) * depth, depth)
        out_ref[...] = coefs_ref[:, :, pl.ds(first, depth)]


def sums_kernel(chunks, n_a, n_b, where_ref, tilts_ref, starts_ref, *refs):
    n = len(chunks)
    *refs, limits_ref = refs
    value_refs = refs[: -4 - n]
    start_ref, *out_refs = refs[-4 - n : -3]
    high_ref, low_ref, spread_ref = refs[-3:]
    limits_ref[...] = turned(tilts_ref)
    n_z = len(value_refs) // 2
    _, rows, depth = value_refs[0].shape
    cols = starts_ref.shape[2]
    half = n_z * rows
    blocks = half // TILE
    base, z, at_a, at_b, core = (where_ref[k] for k in range(5))
    for col in range(n_a * n_b):
        owner = col * cols // rows
        place = jnp.where(core == owner % 2, 0, half) + (owner // 2 * rows + col * cols % rows)
        start_ref[pl.ds(pl.multiple_of(place, 32), cols), :] = starts_ref[col].T
    wave_x, wave_z = waves(base + lax.broadcasted_iota(jnp.int32, (1, depth), 1))
    upper = wave_z >= 0
    need = 16 * jnp.abs(wave_z)
    row_x, row_z = waves(base + lax.broadcasted_iota(jnp.int32, (depth, SLOTS), 0))
    slot = lax.broadcasted_iota(jnp.int32, (depth, SLOTS), 1)
    reach = jnp.where(slot < 64, slot, slot - 64).astype(jnp.float32) * row_x
    table = (16 * jnp.abs(row_z) <= reach) & ((row_z >= 0) == (slot < 64))
    table = jnp.where(table, 1.0, 0.0).astype(jnp.bfloat16)

    for k, ref in enumerate(value_refs):
        side, back = divmod(k, n_z)
        part = jnp.bitwise_and(z - back, n_z - 1) * rows
        start = pl.multiple_of(side * half + part, 64)
        tilt = limits_ref[pl.ds(pl.multiple_of(2 * part + jnp.bitwise_xor(core, side) * rows, 64), rows), :]
        limit = jnp.where(upper, tilt[:, 1:2], tilt[:, 0:1]) * wave_x
        keep = need <= limit
        energy = None
        for comp in range(2):
            value = jnp.where(keep, ref[comp], 0.0)
            high, low = halves(value)
            high_ref[pl.ds(start, rows), comp * depth : (comp + 1) * depth] = high
            low_ref[pl.ds(start, rows), comp * depth : (comp + 1) * depth] = low
            square = value * value
            energy = square if energy is None else energy + square
        if side == 0:
            high, low = halves(energy)
            spread = dot(high, table, (1, 0)) + dot(low, table, (1, 0))
            spread_ref[pl.ds(pl.multiple_of(part, 64), rows), :] = spread

    place = places(blocks, chunks, n_a, n_b)

    def store(name, value):
        if name in place:
            chunk, q_a, q_b, k = place[name]
            a = jnp.bitwise_and(q_a - at_a, n_a - 1)
            b = jnp.bitwise_and(q_b - at_b, n_b - 1)
            out_refs[chunk][a, b, k * TILE : (k + 1) * TILE, :] = value

    for a in range(blocks):
        store(("spread", a, 0), spread_ref[a * TILE : (a + 1) * TILE, :])
    wide = 2 * TILE
    for side, name in ((1, "cross"), (0, "own")):
        for a, b in pairs(half // wide):
            left = slice(a * wide, (a + 1) * wide)
            right = slice(side * half + b * wide, side * half + (b + 1) * wide)
            numer = product(
                (high_ref[left, :], low_ref[left, :]), (high_ref[right, :], low_ref[right, :]), (1, 1)
            )
            for i in range(2):
                for j in range(2):
                    cut = numer[i * TILE : (i + 1) * TILE, j * TILE : (j + 1) * TILE]
                    store((name, 2 * a + i, 2 * b + j), cut)


def matrix_kernel(chunks, shared, n_a, n_b, where_ref, tilts_ref, *refs):
    n = len(chunks)
    own_refs = [refs[c * n_a : (c + 1) * n_a] for c in range(n)]
    partner_refs = [refs[(n + c) * n_a : (n + c + 1) * n_a] for c in range(shared)]
    start_ref, high_ref, low_ref, block_ref, wide_ref = refs[(n + shared) * n_a : (n + shared) * n_a + 5]
    *refs, limits_ref = refs
    limits_ref[...] = turned(tilts_ref)
    spread_ref, hot_ref, *whole_refs = refs[(n + shared) * n_a + 5 :]
    half, total = high_ref.shape
    blocks = half // TILE
    rows, cols = block_ref.shape
    at_a, at_b, core, first, pick_at = (where_ref[k] for k in range(2, 7))
    for side, sources in enumerate((own_refs, partner_refs)):
        here_a, here_b = (at_a, at_b) if side == 0 else (at_b, at_a)
        for chunk, arrays in enumerate(sources):
            whole_ref = whole_refs[side * n + chunk]
            for a, array in enumerate(arrays):
                for b in range(n_b):
                    slot = jnp.bitwise_and(here_a - a, n_a - 1) * n_b + jnp.bitwise_and(here_b - b, n_b - 1)
                    whole_ref[slot] = array[b]
    place = places(blocks, chunks, n_a, n_b)

    def tile(side, *name):
        chunk, q_a, q_b, k = place[name]
        return whole_refs[side * n + chunk][q_a * n_b + q_b, k * TILE : (k + 1) * TILE, :]

    slot = lax.broadcasted_iota(jnp.int32, (rows, SLOTS), 1).astype(jnp.float32)
    for side in range(2):
        for part in range(half // rows):
            tilt = limits_ref[pl.ds(pl.multiple_of((2 * part + jnp.bitwise_xor(core, side)) * rows, 64), rows), :]
            hot = (slot == tilt[:, 1:2]) | (slot == tilt[:, 0:1] + 64)
            hot = jnp.where(hot, 1.0, 0.0).astype(jnp.bfloat16)
            lines = slice(side * half + part * rows, side * half + (part + 1) * rows)
            hot_ref[lines, :SLOTS] = hot
            hot_ref[lines, SLOTS:] = hot
    for b in range(2 * blocks):
        high, low = halves(tile(b // blocks, "spread", b % blocks, 0))
        spread_ref[b * TILE : (b + 1) * TILE, :SLOTS] = high
        spread_ref[b * TILE : (b + 1) * TILE, SLOTS:] = low
    for a in range(blocks):
        lines = slice(a * TILE, (a + 1) * TILE)
        scale = dot(spread_ref[lines, :], hot_ref[...], (1, 1)) * dot(hot_ref[lines, :], spread_ref[...], (1, 1)) + EPS
        guess = lax.rsqrt(scale)
        guess = guess * (1.5 - 0.5 * (scale * guess) * guess)
        for b in range(2 * blocks):
            if b < blocks:
                numer = tile(0, "own", a, b) if a <= b else tile(0, "own", b, a).T
            else:
                numer = tile(0, "cross", a, b - blocks) if a <= b - blocks else tile(1, "cross", b - blocks, a).T
            across = slice(b * TILE, (b + 1) * TILE)
            high, low = halves(numer * guess[:, across])
            high_ref[lines, across] = high
            low_ref[lines, across] = low
    first = pl.multiple_of(first, 64)
    pick = lax.broadcasted_iota(jnp.int32, (total, TILE), 0) == (
        lax.broadcasted_iota(jnp.int32, (total, TILE), 1) + pick_at
    )
    pick = jnp.where(pick, 1.0, 0.0).astype(jnp.bfloat16)
    picked = dot(high_ref[pl.ds(first, rows), :], pick, (1, 0)) + dot(low_ref[pl.ds(first, rows), :], pick, (1, 0))
    block_ref[...] = picked[:, :cols]
    wide_ref[...] = product((high_ref[...], low_ref[...]), halves(start_ref[...]), (1, 0))


def inverse_factor(gram):
    size = gram.shape[0]
    columns = [jnp.broadcast_to(gram[j // 8 * 8 :, j : j + 1], (size - j // 8 * 8, TILE)) for j in range(size)]
    inverse = jnp.where(
        lax.broadcasted_iota(jnp.int32, (size, TILE), 0) == lax.broadcasted_iota(jnp.int32, (size, TILE), 1), 1.0, 0.0
    )
    rows = lax.broadcasted_iota(jnp.int32, (size, TILE), 0)
    for k in range(size):
        base = k // 8 * 8
        pivot = jnp.broadcast_to(columns[k][k - base : k - base + 1, :], (8, TILE))
        root = lax.rsqrt(pivot)
        root = root * (1.5 - 0.5 * (pivot * root) * root)
        scaled = columns[k] * jnp.broadcast_to(root[:1], columns[k].shape)
        line = inverse[k : k + 1, :] * root[:1]
        below = jnp.where(rows[base:] > k, scaled, 0.0)
        tail = inverse[base:] - below * line
        tail = jnp.where(rows[base:] == k, line, tail)
        inverse = jnp.concatenate([inverse[:base], tail], axis=0) if base else tail
        for j in range(k + 1, size):
            shift = j // 8 * 8 - base
            columns[j] = columns[j] - scaled[shift:] * scaled[j - base : j - base + 1, :]
    return inverse[:, :size]


def inverse_of(own, other):
    return inverse_factor(dot(own, own, (0, 0), HIGH) + dot(other, other, (0, 0), HIGH))


def step_kernel(high_ref, low_ref, own_ref, other_ref, wide_ref):
    half = own_ref.shape[0]
    own, other = own_ref[...], other_ref[...]
    inverse = inverse_of(own, other)
    own, other = dot(own, inverse, (1, 1), HIGH), dot(other, inverse, (1, 1), HIGH)
    total = 0.0
    for part, cols in ((own, slice(0, half)), (other, slice(half, 2 * half))):
        total = total + product((high_ref[:, cols], low_ref[:, cols]), halves(part), (1, 0))
    wide_ref[...] = total


def last_kernel(where_ref, own_ref, other_ref, out_ref):
    half = own_ref.shape[0]
    cols = out_ref.shape[1]
    inverse = inverse_of(own_ref[...], other_ref[...])
    first = pl.multiple_of(lax.rem(where_ref[6], half), 32)
    rows = jnp.where(where_ref[6] < half, own_ref[pl.ds(first, cols), :], other_ref[pl.ds(first, cols), :])
    out_ref[...] = dot(rows, inverse, (1, 1), HIGH).T * math.sqrt(2 * half)


def call(body, name, out, inputs, scratch=(), flops=10**9, smem=0, vmem=8):
    here = pl.BlockSpec(memory_space=pltpu.VMEM)
    specs = [pl.BlockSpec(memory_space=pltpu.SMEM)] * smem + [here] * (len(inputs) - smem)
    return pl.pallas_call(
        body,
        name=name,
        out_shape=out,
        in_specs=specs,
        out_specs=jax.tree.map(lambda _: here, out),
        scratch_shapes=list(scratch),
        compiler_params=pltpu.CompilerParams(vmem_limit_bytes=vmem * 1024 * 1024),
        cost_estimate=pl.CostEstimate(flops=flops, bytes_accessed=10**7, transcendentals=0),
    )(*inputs)


def local(coefs, tilts, start_basis, n_z, n_a):
    _, rows, width = coefs.shape
    cols, eig = start_basis.shape
    n_b = n_a
    n_row, n_col = 2 * n_z, n_a * n_b
    total = rows * n_row
    half = total // 2
    depth = width // n_z
    blocks = half // TILE
    f32 = functools.partial(jax.ShapeDtypeStruct, dtype=jnp.float32)
    bf16 = functools.partial(jax.ShapeDtypeStruct, dtype=jnp.bfloat16)
    row = lax.axis_index("row")
    col = lax.axis_index("col")
    z, core = row // 2, row % 2
    y, x = col // n_a, col % n_a
    at_a = jnp.where(core == 0, x, y)
    at_b = jnp.where(core == 0, y, x)

    def device(d, c, q_a, q_b):
        q_a, q_b = q_a % n_a, q_b % n_b
        return (2 * (d % n_z) + c) * n_col + (q_b * n_a + q_a if c == 0 else q_a * n_b + q_b)

    everywhere = [(d, c, a, b) for d in range(n_z) for c in range(2) for a in range(n_a) for b in range(n_b)]

    def send(array, step_a=0, step_b=0, step_z=0):
        perm = [(device(d, c, a, b), device(d + step_z, c, a + step_a, b + step_b)) for d, c, a, b in everywhere]
        return lax.ppermute(array, ("row", "col"), sorted(perm))

    def other_core(array):
        return lax.ppermute(array, "row", [(a, a ^ 1) for a in range(n_row)])

    steps = ORDER
    owner = (col * cols) // rows
    place = jnp.where(owner % 2 == core, 0, half) + (owner // 2) * rows + (col * cols) % rows
    where = jnp.stack([col * width + z * depth, z, at_a, at_b, core, z * rows, place])
    cut = call(split_kernel, "split", [f32((2, rows, depth))] * n_z, (where, coefs), smem=1, vmem=12)
    limits = tilts.T
    mine = [cut[0]] + [None] * (n_z - 1)
    for k in steps:
        mine[k] = send(cut[k], step_z=k)
    starts = jnp.broadcast_to(start_basis.T, (n_col, eig, cols))
    starts = lax.all_to_all(starts, "col", split_axis=0, concat_axis=0, tiled=True)
    theirs = [other_core(mine[0])]
    *mine[1:], starts = lax.optimization_barrier((*mine[1:], starts))
    theirs += [other_core(array) for array in mine[1:]]
    outs = [f32((total, eig))] + [f32((n_a, n_b, per * TILE, TILE)) for per in CHUNKS]
    start, *sums = call(
        functools.partial(sums_kernel, CHUNKS, n_a, n_b),
        "sums",
        outs,
        (where, limits, starts, *mine, *theirs),
        (
            pltpu.VMEM((total, 2 * depth), jnp.bfloat16),
            pltpu.VMEM((total, 2 * depth), jnp.bfloat16),
            pltpu.VMEM((half, SLOTS), jnp.float32),
            pltpu.VMEM((total, 8), jnp.float32),
        ),
        vmem=24,
        smem=1,
    )
    gathered, partner = [], []
    arrived = [[send(part[k], step_a=k) for k in steps] for part in sums]
    for chunk, part in enumerate(sums):
        summed = part[0] + sum(arrived[chunk])
        summed = summed[0] + sum(send(summed[k], step_b=k) for k in steps)
        summed = summed + sum(send(summed, step_z=k) for k in steps)
        near = [summed] + [None] * (n_b - 1)
        for k in steps:
            near[k] = send(summed, step_b=k)
        near = jnp.stack(near)
        far = [near] + [None] * (n_a - 1)
        for k in steps:
            far[k] = send(near, step_a=k)
        gathered += far
        if chunk < SHARED:
            partner += [other_core(array) for array in far]
    whole = [pltpu.VMEM((n_col, per * TILE, TILE), jnp.float32) for per in CHUNKS]
    high, low, block, own = call(
        functools.partial(matrix_kernel, CHUNKS, SHARED, n_a, n_b),
        "matrix",
        (bf16((half, total)), bf16((half, total)), f32((rows, cols)), f32((half, eig))),
        (where, limits, *gathered, *partner, start),
        (
            pltpu.VMEM((total, 2 * SLOTS), jnp.bfloat16),
            pltpu.VMEM((total, 2 * SLOTS), jnp.bfloat16),
            *whole,
            *whole[:SHARED],
            pltpu.VMEM((total, 8), jnp.float32),
        ),
        vmem=28,
        smem=1,
    )
    other = other_core(own)
    for _ in range(ITERS - 1):
        own = call(step_kernel, "step", f32((half, eig)), (high, low, own, other))
        other = other_core(own)
    basis = call(last_kernel, "last", f32((eig, cols)), (where, own, other), smem=1)
    return (block, basis.T)


def solution(mesh):
    n_z = mesh.shape["row"] // 2
    side = math.isqrt(mesh.shape["col"])
    in_specs = (P(None, "row", "col"), P(), P("col", None))
    out_specs = (P("row", "col"), P("col", None))
    body = functools.partial(local, n_z=n_z, n_a=side)
    return jax.shard_map(body, mesh=mesh, in_specs=in_specs, out_specs=out_specs, check_vma=False)
```

```python
import functools
import math

import jax
import jax.numpy as jnp
from jax import lax
from jax.experimental import pallas as pl
from jax.experimental.pallas import tpu as pltpu
from jax.sharding import PartitionSpec as P

GRID = 32
ITERS = 4
EPS = 1e-06
TILE = 128
SLOTS = 128
CHUNKS = (3,)
SHARED = 1
ORDER = (2, 1, 3)
HIGH = lax.Precision.HIGHEST


def dot(left, right, contract, precision=None):
    dims = (((contract[0],), (contract[1],)), ((), ()))
    return lax.dot_general(left, right, dims, precision=precision, preferred_element_type=jnp.float32)


def halves(array):
    high = array.astype(jnp.bfloat16)
    return high, (array - high.astype(jnp.float32)).astype(jnp.bfloat16)


def product(left, right, contract):
    total = dot(left[0], right[1], contract) + dot(left[1], right[0], contract)
    return total + dot(left[0], right[0], contract)


def turned(ref):
    rows = ref[...].astype(jnp.float32)
    return jnp.concatenate([rows] * 4, axis=0).T


def waves(index):
    wave_x = jnp.abs(lax.shift_right_arithmetic(index, 9) - GRID // 2)
    wave_z = jnp.bitwise_and(index, GRID - 1) - GRID // 2
    return wave_x.astype(jnp.float32), wave_z.astype(jnp.float32)


def pairs(blocks):
    return [(a, b) for a in range(blocks) for b in range(a, blocks)]


def tile_order(blocks):
    tri = pairs(blocks)
    order = [("cross", *pair) for pair in tri] + [("spread", a, 0) for a in range(blocks)]
    return order + [("own", *pair) for pair in tri]


def places(blocks, chunks, n_a, n_b):
    found, start = {}, 0
    order = tile_order(blocks)
    for chunk, per in enumerate(chunks):
        for k in range(n_a * n_b * per):
            found[order[start + k]] = (chunk, k // (n_b * per), k // per % n_b, k % per)
        start += n_a * n_b * per
    return found


def split_kernel(where_ref, coefs_ref, *out_refs):
    depth = out_refs[0].shape[2]
    for k, out_ref in enumerate(out_refs):
        first = pl.multiple_of(jnp.bitwise_and(where_ref[1] + k, len(out_refs) - 1) * depth, depth)
        out_ref[...] = coefs_ref[:, :, pl.ds(first, depth)]


def sums_kernel(chunks, n_a, n_b, where_ref, tilts_ref, starts_ref, *refs):
    n = len(chunks)
    *refs, limits_ref = refs
    value_refs = refs[: -4 - n]
    start_ref, *out_refs = refs[-4 - n : -3]
    high_ref, low_ref, spread_ref = refs[-3:]
    limits_ref[...] = turned(tilts_ref)
    n_z = len(value_refs) // 2
    _, rows, depth = value_refs[0].shape
    cols = starts_ref.shape[2]
    half = n_z * rows
    blocks = half // TILE
    base, z, at_a, at_b, core = (where_ref[k] for k in range(5))
    for col in range(n_a * n_b):
        owner = col * cols // rows
        place = jnp.where(core == owner % 2, 0, half) + (owner // 2 * rows + col * cols % rows)
        start_ref[pl.ds(pl.multiple_of(place, 32), cols), :] = starts_ref[col].T
    wave_x, wave_z = waves(base + lax.broadcasted_iota(jnp.int32, (1, depth), 1))
    upper = wave_z >= 0
    need = 16 * jnp.abs(wave_z)
    row_x, row_z = waves(base + lax.broadcasted_iota(jnp.int32, (depth, SLOTS), 0))
    slot = lax.broadcasted_iota(jnp.int32, (depth, SLOTS), 1)
    reach = jnp.where(slot < 64, slot, slot - 64).astype(jnp.float32) * row_x
    table = (16 * jnp.abs(row_z) <= reach) & ((row_z >= 0) == (slot < 64))
    table = jnp.where(table, 1.0, 0.0).astype(jnp.bfloat16)

    for k, ref in enumerate(value_refs):
        side, back = divmod(k, n_z)
        part = jnp.bitwise_and(z - back, n_z - 1) * rows
        start = pl.multiple_of(side * half + part, 64)
        tilt = limits_ref[pl.ds(pl.multiple_of(2 * part + jnp.bitwise_xor(core, side) * rows, 64), rows), :]
        limit = jnp.where(upper, tilt[:, 1:2], tilt[:, 0:1]) * wave_x
        keep = need <= limit
        energy = None
        for comp in range(2):
            value = jnp.where(keep, ref[comp], 0.0)
            high, low = halves(value)
            high_ref[pl.ds(start, rows), comp * depth : (comp + 1) * depth] = high
            low_ref[pl.ds(start, rows), comp * depth : (comp + 1) * depth] = low
            square = value * value
            energy = square if energy is None else energy + square
        if side == 0:
            high, low = halves(energy)
            spread = dot(high, table, (1, 0)) + dot(low, table, (1, 0))
            spread_ref[pl.ds(pl.multiple_of(part, 64), rows), :] = spread

    place = places(blocks, chunks, n_a, n_b)

    def store(name, value):
        if name in place:
            chunk, q_a, q_b, k = place[name]
            a = jnp.bitwise_and(q_a - at_a, n_a - 1)
            b = jnp.bitwise_and(q_b - at_b, n_b - 1)
            out_refs[chunk][a, b, k * TILE : (k + 1) * TILE, :] = value

    for a in range(blocks):
        store(("spread", a, 0), spread_ref[a * TILE : (a + 1) * TILE, :])
    wide = 2 * TILE
    for side, name in ((1, "cross"), (0, "own")):
        for a, b in pairs(half // wide):
            left = slice(a * wide, (a + 1) * wide)
            right = slice(side * half + b * wide, side * half + (b + 1) * wide)
            numer = product(
                (high_ref[left, :], low_ref[left, :]), (high_ref[right, :], low_ref[right, :]), (1, 1)
            )
            for i in range(2):
                for j in range(2):
                    cut = numer[i * TILE : (i + 1) * TILE, j * TILE : (j + 1) * TILE]
                    store((name, 2 * a + i, 2 * b + j), cut)


def matrix_kernel(chunks, shared, n_a, n_b, where_ref, tilts_ref, *refs):
    n = len(chunks)
    own_refs = [refs[2 * c * n_a : 2 * (c + 1) * n_a] for c in range(n)]
    partner_refs = [refs[2 * (n + c) * n_a : 2 * (n + c + 1) * n_a] for c in range(shared)]
    start_ref, high_ref, low_ref, block_ref, wide_ref = refs[2 * (n + shared) * n_a : 2 * (n + shared) * n_a + 5]
    *refs, limits_ref = refs
    limits_ref[...] = turned(tilts_ref)
    spread_ref, hot_ref, *whole_refs = refs[2 * (n + shared) * n_a + 5 :]
    half, total = high_ref.shape
    blocks = half // TILE
    rows, cols = block_ref.shape
    at_a, at_b, core, first, pick_at = (where_ref[k] for k in range(2, 7))
    for side, sources in enumerate((own_refs, partner_refs)):
        here_a, here_b = (at_a, at_b) if side == 0 else (at_b, at_a)
        for chunk, arrays in enumerate(sources):
            whole_ref = whole_refs[side * n + chunk]
            for a in range(n_a):
                for b in range(n_b):
                    value = arrays[a][...] if b == 0 else arrays[n_a + a][b - 1]
                    slot = jnp.bitwise_and(here_a - a, n_a - 1) * n_b + jnp.bitwise_and(here_b - b, n_b - 1)
                    whole_ref[slot] = value
    place = places(blocks, chunks, n_a, n_b)

    def tile(side, *name):
        chunk, q_a, q_b, k = place[name]
        return whole_refs[side * n + chunk][q_a * n_b + q_b, k * TILE : (k + 1) * TILE, :]

    slot = lax.broadcasted_iota(jnp.int32, (rows, SLOTS), 1).astype(jnp.float32)
    for side in range(2):
        for part in range(half // rows):
            tilt = limits_ref[pl.ds(pl.multiple_of((2 * part + jnp.bitwise_xor(core, side)) * rows, 64), rows), :]
            hot = (slot == tilt[:, 1:2]) | (slot == tilt[:, 0:1] + 64)
            hot = jnp.where(hot, 1.0, 0.0).astype(jnp.bfloat16)
            lines = slice(side * half + part * rows, side * half + (part + 1) * rows)
            hot_ref[lines, :SLOTS] = hot
            hot_ref[lines, SLOTS:] = hot
    for b in range(2 * blocks):
        high, low = halves(tile(b // blocks, "spread", b % blocks, 0))
        spread_ref[b * TILE : (b + 1) * TILE, :SLOTS] = high
        spread_ref[b * TILE : (b + 1) * TILE, SLOTS:] = low
    for a in range(blocks):
        lines = slice(a * TILE, (a + 1) * TILE)
        scale = dot(spread_ref[lines, :], hot_ref[...], (1, 1)) * dot(hot_ref[lines, :], spread_ref[...], (1, 1)) + EPS
        guess = lax.rsqrt(scale)
        guess = guess * (1.5 - 0.5 * (scale * guess) * guess)
        for b in range(2 * blocks):
            if b < blocks:
                numer = tile(0, "own", a, b) if a <= b else tile(0, "own", b, a).T
            else:
                numer = tile(0, "cross", a, b - blocks) if a <= b - blocks else tile(1, "cross", b - blocks, a).T
            across = slice(b * TILE, (b + 1) * TILE)
            high, low = halves(numer * guess[:, across])
            high_ref[lines, across] = high
            low_ref[lines, across] = low
    first = pl.multiple_of(first, 64)
    pick = lax.broadcasted_iota(jnp.int32, (total, TILE), 0) == (
        lax.broadcasted_iota(jnp.int32, (total, TILE), 1) + pick_at
    )
    pick = jnp.where(pick, 1.0, 0.0).astype(jnp.bfloat16)
    picked = dot(high_ref[pl.ds(first, rows), :], pick, (1, 0)) + dot(low_ref[pl.ds(first, rows), :], pick, (1, 0))
    block_ref[...] = picked[:, :cols]
    wide_ref[...] = product((high_ref[...], low_ref[...]), halves(start_ref[...]), (1, 0))


def inverse_factor(gram):
    size = gram.shape[0]
    columns = [jnp.broadcast_to(gram[j // 8 * 8 :, j : j + 1], (size - j // 8 * 8, TILE)) for j in range(size)]
    inverse = jnp.where(
        lax.broadcasted_iota(jnp.int32, (size, TILE), 0) == lax.broadcasted_iota(jnp.int32, (size, TILE), 1), 1.0, 0.0
    )
    rows = lax.broadcasted_iota(jnp.int32, (size, TILE), 0)
    for k in range(size):
        base = k // 8 * 8
        pivot = jnp.broadcast_to(columns[k][k - base : k - base + 1, :], (8, TILE))
        root = lax.rsqrt(pivot)
        root = root * (1.5 - 0.5 * (pivot * root) * root)
        scaled = columns[k] * jnp.broadcast_to(root[:1], columns[k].shape)
        line = inverse[k : k + 1, :] * root[:1]
        below = jnp.where(rows[base:] > k, scaled, 0.0)
        tail = inverse[base:] - below * line
        tail = jnp.where(rows[base:] == k, line, tail)
        inverse = jnp.concatenate([inverse[:base], tail], axis=0) if base else tail
        for j in range(k + 1, size):
            shift = j // 8 * 8 - base
            columns[j] = columns[j] - scaled[shift:] * scaled[j - base : j - base + 1, :]
    return inverse[:, :size]


def inverse_of(own, other):
    return inverse_factor(dot(own, own, (0, 0), HIGH) + dot(other, other, (0, 0), HIGH))


def step_kernel(high_ref, low_ref, own_ref, other_ref, wide_ref):
    half = own_ref.shape[0]
    own, other = own_ref[...], other_ref[...]
    inverse = inverse_of(own, other)
    own, other = dot(own, inverse, (1, 1), HIGH), dot(other, inverse, (1, 1), HIGH)
    total = 0.0
    for part, cols in ((own, slice(0, half)), (other, slice(half, 2 * half))):
        total = total + product((high_ref[:, cols], low_ref[:, cols]), halves(part), (1, 0))
    wide_ref[...] = total


def last_kernel(where_ref, own_ref, other_ref, out_ref):
    half = own_ref.shape[0]
    cols = out_ref.shape[1]
    inverse = inverse_of(own_ref[...], other_ref[...])
    first = pl.multiple_of(lax.rem(where_ref[6], half), 32)
    rows = jnp.where(where_ref[6] < half, own_ref[pl.ds(first, cols), :], other_ref[pl.ds(first, cols), :])
    out_ref[...] = dot(rows, inverse, (1, 1), HIGH).T * math.sqrt(2 * half)


def call(body, name, out, inputs, scratch=(), flops=10**9, smem=0, vmem=8):
    here = pl.BlockSpec(memory_space=pltpu.VMEM)
    specs = [pl.BlockSpec(memory_space=pltpu.SMEM)] * smem + [here] * (len(inputs) - smem)
    return pl.pallas_call(
        body,
        name=name,
        out_shape=out,
        in_specs=specs,
        out_specs=jax.tree.map(lambda _: here, out),
        scratch_shapes=list(scratch),
        compiler_params=pltpu.CompilerParams(vmem_limit_bytes=vmem * 1024 * 1024),
        cost_estimate=pl.CostEstimate(flops=flops, bytes_accessed=10**7, transcendentals=0),
    )(*inputs)


def local(coefs, tilts, start_basis, n_z, n_a):
    _, rows, width = coefs.shape
    cols, eig = start_basis.shape
    n_b = n_a
    n_row, n_col = 2 * n_z, n_a * n_b
    total = rows * n_row
    half = total // 2
    depth = width // n_z
    blocks = half // TILE
    f32 = functools.partial(jax.ShapeDtypeStruct, dtype=jnp.float32)
    bf16 = functools.partial(jax.ShapeDtypeStruct, dtype=jnp.bfloat16)
    row = lax.axis_index("row")
    col = lax.axis_index("col")
    z, core = row // 2, row % 2
    y, x = col // n_a, col % n_a
    at_a = jnp.where(core == 0, x, y)
    at_b = jnp.where(core == 0, y, x)

    def device(d, c, q_a, q_b):
        q_a, q_b = q_a % n_a, q_b % n_b
        return (2 * (d % n_z) + c) * n_col + (q_b * n_a + q_a if c == 0 else q_a * n_b + q_b)

    everywhere = [(d, c, a, b) for d in range(n_z) for c in range(2) for a in range(n_a) for b in range(n_b)]

    def send(array, step_a=0, step_b=0, step_z=0):
        perm = [(device(d, c, a, b), device(d + step_z, c, a + step_a, b + step_b)) for d, c, a, b in everywhere]
        return lax.ppermute(array, ("row", "col"), sorted(perm))

    def other_core(array):
        return lax.ppermute(array, "row", [(a, a ^ 1) for a in range(n_row)])

    steps = ORDER
    owner = (col * cols) // rows
    place = jnp.where(owner % 2 == core, 0, half) + (owner // 2) * rows + (col * cols) % rows
    where = jnp.stack([col * width + z * depth, z, at_a, at_b, core, z * rows, place])
    cut = call(split_kernel, "split", [f32((2, rows, depth))] * n_z, (where, coefs), smem=1, vmem=12)
    limits = tilts.T
    mine = [cut[0]] + [None] * (n_z - 1)
    for k in steps:
        mine[k] = send(cut[k], step_z=k)
    starts = jnp.broadcast_to(start_basis.T, (n_col, eig, cols))
    starts = lax.all_to_all(starts, "col", split_axis=0, concat_axis=0, tiled=True)
    theirs = [other_core(mine[0])]
    *mine[1:], starts = lax.optimization_barrier((*mine[1:], starts))
    theirs += [other_core(array) for array in mine[1:]]
    outs = [f32((total, eig))] + [f32((n_a, n_b, per * TILE, TILE)) for per in CHUNKS]
    start, *sums = call(
        functools.partial(sums_kernel, CHUNKS, n_a, n_b),
        "sums",
        outs,
        (where, limits, starts, *mine, *theirs),
        (
            pltpu.VMEM((total, 2 * depth), jnp.bfloat16),
            pltpu.VMEM((total, 2 * depth), jnp.bfloat16),
            pltpu.VMEM((half, SLOTS), jnp.float32),
            pltpu.VMEM((total, 8), jnp.float32),
        ),
        vmem=24,
        smem=1,
    )
    gathered, partner = [], []
    arrived = [[send(part[k], step_a=k) for k in steps] for part in sums]
    for chunk, part in enumerate(sums):
        summed = part[0] + sum(arrived[chunk])
        summed = summed[0] + sum(send(summed[k], step_b=k) for k in steps)
        summed = summed + sum(send(summed, step_z=k) for k in steps)
        others = [None] * (n_b - 1)
        for k in steps:
            others[k - 1] = send(summed, step_b=k)
        near = [summed] + [None] * (n_a - 1)
        for k in steps:
            near[k] = send(summed, step_a=k)
        others = jnp.stack(others)
        far = [others] + [None] * (n_a - 1)
        for k in steps:
            far[k] = send(others, step_a=k)
        gathered += near + far
        if chunk < SHARED:
            partner += [other_core(array) for array in near + far]
    whole = [pltpu.VMEM((n_col, per * TILE, TILE), jnp.float32) for per in CHUNKS]
    high, low, block, own = call(
        functools.partial(matrix_kernel, CHUNKS, SHARED, n_a, n_b),
        "matrix",
        (bf16((half, total)), bf16((half, total)), f32((rows, cols)), f32((half, eig))),
        (where, limits, *gathered, *partner, start),
        (
            pltpu.VMEM((total, 2 * SLOTS), jnp.bfloat16),
            pltpu.VMEM((total, 2 * SLOTS), jnp.bfloat16),
            *whole,
            *whole[:SHARED],
            pltpu.VMEM((total, 8), jnp.float32),
        ),
        vmem=28,
        smem=1,
    )
    other = other_core(own)
    for _ in range(ITERS - 1):
        own = call(step_kernel, "step", f32((half, eig)), (high, low, own, other))
        other = other_core(own)
    basis = call(last_kernel, "last", f32((eig, cols)), (where, own, other), smem=1)
    return (block, basis.T)


def solution(mesh):
    n_z = mesh.shape["row"] // 2
    side = math.isqrt(mesh.shape["col"])
    in_specs = (P(None, "row", "col"), P(), P("col", None))
    out_specs = (P("row", "col"), P("col", None))
    body = functools.partial(local, n_z=n_z, n_a=side)
    return jax.shard_map(body, mesh=mesh, in_specs=in_specs, out_specs=out_specs, check_vma=False)
```
